32 devices in a mesh: dp: 1, tp: 32 (over x, y, z, core).
Axes of the slice: x: 2, y: 2, z: 4, core: 2. Of those that a mesh axis runs over, the one named last changes fastest.
Arguments:
- x: bfloat16 [2048, 4608], P('dp')
- w_gate: bfloat16 [4608, 36864], P(None, 'tp')
- w_up: bfloat16 [4608, 36864], P(None, 'tp')
- w_down: bfloat16 [36864, 4608], P('tp')
Outputs:
- output: bfloat16 [2048, 4608], P('dp')
All inputs are finite; a program needn't handle non-finite values.
Results may differ from the reference program's by a relative error of at most 0.016.
Values are sent between devices in bfloat16 or wider.
A program may use at most 2 GiB of HBM per device.

```python
import jax
import jax.numpy as jnp

ROWS = 2048
D = 4608
FF = 36864


def setup_inputs(seed: int = 0, part: int = 0) -> dict:
    kx, kg, ku, kd = jax.random.split(jax.random.key(seed), 4)
    drawn = {
        "x": jax.random.normal(jax.random.fold_in(kx, part), (ROWS, D), jnp.float32),
        "w_gate": jax.random.normal(kg, (D, FF), jnp.float32) * D**-0.5,
        "w_up": jax.random.normal(ku, (D, FF), jnp.float32) * D**-0.5,
        "w_down": jax.random.normal(kd, (FF, D), jnp.float32) * FF**-0.5,
    }
    return {k: v.astype(jnp.bfloat16) for k, v in drawn.items()}


def reference(x, w_gate, w_up, w_down):
    gate = jnp.dot(x, w_gate, preferred_element_type=jnp.float32)
    up = jnp.dot(x, w_up, preferred_element_type=jnp.float32)
    hidden = (jax.nn.gelu(gate) * up).astype(jnp.bfloat16)
    return jnp.dot(hidden, w_down, preferred_element_type=jnp.float32).astype(jnp.bfloat16)
```

```python
import functools

import jax
import jax.numpy as jnp
from jax import lax
from jax.experimental import pallas as pl
from jax.experimental.pallas import tpu as pltpu
from jax.sharding import PartitionSpec as P

MESH = pl.DeviceIdType.MESH
F32, BF16 = jnp.float32, jnp.bfloat16

R = 128
LAST = 10

A_BLOCKS = (5, 5)
B_BLOCKS = (4, 4)


def kernel(dims, x_ref, wg_ref, wu_ref, wd_ref, y_ref,
           wgu, wdv, xb, hb, tb, stg, fin, rx1, rx2, rz1, rz2, rbz, rbm, rb1, rb2,
           wsem, xsem, ysem, ss, rs):
    rows, d, ff = dims
    n = rows // R
    half = d // 2
    nb = ff // 128
    W = tb.shape[0]
    me = lax.axis_index("tp")
    c = lax.rem(me, 2)
    z = lax.rem(me // 2, 4)
    yy = lax.rem(me // 8, 2)
    xx = me // 16

    def dev(px, py, pz, pc):
        return ((px * 2 + py) * 4 + pz) * 2 + pc

    xp = dev(1 - xx, yy, z, c)
    yp = dev(xx, 1 - yy, z, c)
    cp = dev(xx, yy, z, 1 - c)
    is_mid = (z == 1) | (z == 2)
    is_end = (z == 0) | (z == 3)
    m = z // 2
    om = dev(xx, yy, 3 - z, c)
    ez = dev(xx, yy, 3 * m, c)
    mz = dev(xx, yy, 1 + m, c)

    ids = {}

    def rc(name, k, src, dst, to):
        i = ids.setdefault(name, len(ids))
        return pltpu.make_async_remote_copy(
            src_ref=src, dst_ref=dst, send_sem=ss.at[i, k], recv_sem=rs.at[i, k],
            device_id={"tp": to}, device_id_type=MESH)

    def wcopy(i, part):
        src = (wg_ref, wu_ref)[part].at[:, pl.ds(i * 128, 128)]
        return pltpu.make_async_copy(src, wgu.at[i, :, pl.ds(part * 128, 128)], wsem.at[2 * i + part])

    def xcopy(k):
        return pltpu.make_async_copy(
            x_ref.at[pl.ds(pl.multiple_of(k * R, R), R), :], xb.at[lax.rem(k, 2)], xsem.at[lax.rem(k, 2)])

    def wd_own():
        return pltpu.make_async_copy(
            wd_ref.at[:, pl.ds(pl.multiple_of(c * half, 128), half)], wdv.at[pl.ds(0, ff)], wsem.at[2 * nb])

    def wd_part():
        return rc("wd", 0, wd_ref.at[:, pl.ds(pl.multiple_of((1 - c) * half, 128), half)],
                  wdv.at[pl.ds(ff, ff)], cp)

    xcopy(0).start()
    for i in range(nb):
        for part in range(2):
            wcopy(i, part).start()
    wd_own().start()

    bar = pltpu.get_barrier_semaphore()
    for peer in (xp, yp, cp):
        pl.semaphore_signal(bar, inc=1, device_id={"tp": peer}, device_id_type=MESH)

    @pl.when(is_mid)
    def _():
        pl.semaphore_signal(bar, inc=1, device_id={"tp": om}, device_id_type=MESH)
        pl.semaphore_signal(bar, inc=1, device_id={"tp": ez}, device_id_type=MESH)
        pl.semaphore_wait(bar, 5)

    @pl.when(is_end)
    def _():
        pl.semaphore_signal(bar, inc=1, device_id={"tp": mz}, device_id_type=MESH)
        pl.semaphore_wait(bar, 4)

    wd_part().start()

    A, B = [], []
    off = 0
    for j, blocks in enumerate(A_BLOCKS):
        ax = (xp, xx, yp, yy) if j == 0 else (yp, yy, xp, xx)
        A.append((f"A{j}", off, blocks * 128) + ax)
        off += blocks * 128
    boff = off
    for j, blocks in enumerate(B_BLOCKS):
        ax = (xp, xx, yp, yy) if j == 0 else (yp, yy, xp, xx)
        B.append((f"B{j}", off, blocks * 128) + ax)
        off += blocks * 128
    bw = off - boff
    R2, R4, R8 = R // 2, R // 4, R // 8
    bcols = pl.ds(boff, bw)

    def Y(k, row, nrows, o, w):
        return y_ref.at[pl.ds(pl.multiple_of(k * R + row, 16), nrows),
                        pl.ds(pl.multiple_of(c * half + o, 128), w)]

    def rows_at(start, size):
        return pl.ds(pl.multiple_of(start, 8), size)

    def a_msg(col, k, what):
        nm, o, w, p, a, q, b = col
        s = lax.rem(k, W)
        cols = pl.ds(o, w)
        q0 = a * R2 + b * R4
        key = nm + what
        if what == "xs":
            return rc(key, k, stg.at[s, pl.ds(0, R2), cols], rx1.at[k, :, cols], p)
        if what == "ys":
            return rc(key, k, stg.at[s, pl.ds(R2, R4), cols], rx2.at[k, :, cols], q)
        if what == "ze":
            return rc(key, k, stg.at[s, pl.ds(3 * R4, R4), cols], rz1.at[k, :, cols], mz)
        if what == "zm":
            return rc(key, k, stg.at[s, pl.ds(3 * R4, R8), cols], rz2.at[k, :, cols], om)
        if what == "gm":
            return rc(key, k, fin.at[s, :, cols], Y(k, q0 + m * R8, R8, o, w), om)
        reg = Y(k, q0, R4, o, w)
        if what == "ge":
            return rc(key, k, reg, reg, ez)
        if what == "gy":
            return rc(key, k, reg, reg, q)
        if what == "gx1":
            return rc(key, k, reg, reg, p)
        reg = Y(k, a * R2 + (1 - b) * R4, R4, o, w)
        assert what == "gx2"
        return rc(key, k, reg, reg, p)

    def b_msg(col, k, what):
        nm, o, w, p, a, q, b = col
        s = lax.rem(k, W)
        cols = pl.ds(o, w)
        lc = pl.ds(o - boff, w)
        key = nm + what
        if what == "xs":
            return rc(key, k, stg.at[s, pl.ds(R2, R4), cols], rb1.at[k, :, lc], p)
        if what == "ys":
            return rc(key, k, stg.at[s, pl.ds(3 * R4, R8), cols], rb2.at[k, :, lc], q)
        own = m * R2 + a * R4
        if what == "gy":
            return rc(key, k, fin.at[s, :, cols], Y(k, own + b * R8, R8, o, w), q)
        if what in ("gx", "gm1", "ge1"):
            reg = Y(k, own, R4, o, w)
            return rc(key, k, reg, reg, {"gx": p, "gm1": om, "ge1": ez}[what])
        if what in ("gm2", "ge2"):
            reg = Y(k, m * R2 + (1 - a) * R4, R4, o, w)
            return rc(key, k, reg, reg, {"gm2": om, "ge2": ez}[what])
        row = (1 - m) * R2 + {"ge3": a, "ge4": 1 - a}[what] * R4
        reg = Y(k, row, R4, o, w)
        return rc(key, k, reg, reg, ez)

    def bz_msg(k, what):
        s = lax.rem(k, W)
        if what == "ze":
            return rc("Bze", k, stg.at[s, :, bcols], rbz.at[k], mz)
        return rc("Bzm", k, stg.at[s, pl.ds(0, R2), bcols], rbm.at[k], om)

    def c_msg(k):
        reg = Y(k, 0, R, 0, half)
        return rc("cg", k, reg, reg, cp)

    def h_msg(k):
        sl = lax.rem(k, 4)
        return rc("h", k, hb.at[sl, :, pl.ds(0, ff)], hb.at[sl, :, pl.ds(ff, ff)], cp)

    def ylocal(col, j, k, row):
        nm, o, w = col[:3]
        s = lax.rem(k, W)
        return pltpu.make_async_copy(fin.at[s, :, pl.ds(o, w)], Y(k, row, R8, o, w), ysem.at[j, k])

    def a_fin_row(col):
        return col[4] * R2 + col[6] * R4 + m * R8

    def b_fin_row(col):
        return m * R2 + col[4] * R4 + col[6] * R8

    def h0(k):
        s = lax.rem(k, W)
        for col in A:
            nm, o, w, p, a, q, b = col
            cols = pl.ds(o, w)
            stg[s, pl.ds(0, R2), cols] = tb[s, rows_at((1 - a) * R2, R2), cols].astype(BF16)
            a_msg(col, k, "xs").start()

        @pl.when(is_end)
        def _():
            stg[s, :, bcols] = tb[s, :, bcols].astype(BF16)
            bz_msg(k, "ze").start()

    def h1(k):
        s = lax.rem(k, W)
        for col in A:
            nm, o, w, p, a, q, b = col
            cols = pl.ds(o, w)
            a_msg(col, k, "xs").wait_recv()
            snd, kp = (1 - b) * R4, b * R4
            stg[s, pl.ds(R2, R4), cols] = (
                tb[s, rows_at(a * R2 + snd, R4), cols]
                + rx1[k, rows_at(snd, R4), cols].astype(F32)).astype(BF16)
            a_msg(col, k, "ys").start()
            tb[s, rows_at(a * R2 + kp, R4), cols] += rx1[k, rows_at(kp, R4), cols].astype(F32)

        @pl.when(is_mid)
        def _():
            bz_msg(k, "ze").wait_recv()
            stg[s, pl.ds(0, R2), bcols] = (
                tb[s, rows_at((1 - m) * R2, R2), bcols]
                + rbz[k, rows_at((1 - m) * R2, R2), :].astype(F32)).astype(BF16)
            bz_msg(k, "zm").start()
            tb[s, rows_at(m * R2, R2), bcols] += rbz[k, rows_at(m * R2, R2), :].astype(F32)

    def h2(k):
        s = lax.rem(k, W)
        for col in A:
            nm, o, w, p, a, q, b = col
            cols = pl.ds(o, w)
            a_msg(col, k, "ys").wait_recv()
            q0 = rows_at(a * R2 + b * R4, R4)

            @pl.when(is_end)
            def _():
                stg[s, pl.ds(3 * R4, R4), cols] = (
                    tb[s, q0, cols] + rx2[k, :, cols].astype(F32)).astype(BF16)
                a_msg(col, k, "ze").start()

            @pl.when(is_mid)
            def _():
                tb[s, q0, cols] += rx2[k, :, cols].astype(F32)

        @pl.when(is_mid)
        def _():
            bz_msg(k, "zm").wait_recv()
            for col in B:
                nm, o, w, p, a, q, b = col
                cols, lc = pl.ds(o, w), pl.ds(o - boff, w)
                snd, kp = (1 - a) * R4, a * R4
                stg[s, pl.ds(R2, R4), cols] = (
                    tb[s, rows_at(m * R2 + snd, R4), cols]
                    + rbm[k, rows_at(snd, R4), lc].astype(F32)).astype(BF16)
                b_msg(col, k, "xs").start()
                tb[s, rows_at(m * R2 + kp, R4), cols] += rbm[k, rows_at(kp, R4), lc].astype(F32)

    def h3(k):
        s = lax.rem(k, W)

        @pl.when(is_mid)
        def _():
            for col in A:
                nm, o, w, p, a, q, b = col
                cols = pl.ds(o, w)
                a_msg(col, k, "ze").wait_recv()
                q0 = a * R2 + b * R4
                snd, kp = (1 - m) * R8, m * R8
                stg[s, pl.ds(3 * R4, R8), cols] = (
                    tb[s, rows_at(q0 + snd, R8), cols]
                    + rz1[k, rows_at(snd, R8), cols].astype(F32)).astype(BF16)
                a_msg(col, k, "zm").start()
                tb[s, rows_at(q0 + kp, R8), cols] += rz1[k, rows_at(kp, R8), cols].astype(F32)
            for col in B:
                nm, o, w, p, a, q, b = col
                cols, lc = pl.ds(o, w), pl.ds(o - boff, w)
                b_msg(col, k, "xs").wait_recv()
                q0 = m * R2 + a * R4
                snd, kp = (1 - b) * R8, b * R8
                stg[s, pl.ds(3 * R4, R8), cols] = (
                    tb[s, rows_at(q0 + snd, R8), cols]
                    + rb1[k, rows_at(snd, R8), lc].astype(F32)).astype(BF16)
                b_msg(col, k, "ys").start()
                tb[s, rows_at(q0 + kp, R8), cols] += rb1[k, rows_at(kp, R8), lc].astype(F32)

    def h4(k):
        s = lax.rem(k, W)

        @pl.when(is_mid)
        def _():
            for j, col in enumerate(A):
                nm, o, w, p, a, q, b = col
                cols = pl.ds(o, w)
                a_msg(col, k, "zm").wait_recv()
                fin[s, :, cols] = (
                    tb[s, rows_at(a_fin_row(col), R8), cols] + rz2[k, :, cols].astype(F32)).astype(BF16)
                a_msg(col, k, "gm").start()
                ylocal(col, j, k, a_fin_row(col)).start()
            for j, col in enumerate(B):
                nm, o, w, p, a, q, b = col
                cols, lc = pl.ds(o, w), pl.ds(o - boff, w)
                b_msg(col, k, "ys").wait_recv()
                fin[s, :, cols] = (
                    tb[s, rows_at(b_fin_row(col), R8), cols] + rb2[k, :, lc].astype(F32)).astype(BF16)
                b_msg(col, k, "gy").start()
                ylocal(col, 2 + j, k, b_fin_row(col)).start()

    def h5(k):
        @pl.when(is_mid)
        def _():
            for j, col in enumerate(A):
                ylocal(col, j, k, a_fin_row(col)).wait()
                a_msg(col, k, "gm").wait_recv()
                for what in ("ge", "gy", "gx1"):
                    a_msg(col, k, what).start()
            for j, col in enumerate(B):
                ylocal(col, 2 + j, k, b_fin_row(col)).wait()
                b_msg(col, k, "gy").wait_recv()
                for what in ("gx", "gm1", "ge1"):
                    b_msg(col, k, what).start()
            for col in A:
                for what in ("xs", "ys", "zm", "gm"):
                    a_msg(col, k, what).wait_send()
            bz_msg(k, "zm").wait_send()
            for col in B:
                for what in ("xs", "ys", "gy"):
                    b_msg(col, k, what).wait_send()

        @pl.when(is_end)
        def _():
            for col in A:
                for what in ("xs", "ys", "ze"):
                    a_msg(col, k, what).wait_send()
            bz_msg(k, "ze").wait_send()

    def h6(k):
        @pl.when(is_mid)
        def _():
            for col in A:
                a_msg(col, k, "gy").wait_recv()
                a_msg(col, k, "gx2").start()
            for col in B:
                b_msg(col, k, "gx").wait_recv()
                b_msg(col, k, "gm2").start()
                b_msg(col, k, "ge2").start()

        @pl.when(is_end)
        def _():
            for col in A:
                a_msg(col, k, "ge").wait_recv()
                a_msg(col, k, "gy").start()
                a_msg(col, k, "gx1").start()

    def h7(k):
        @pl.when(is_mid)
        def _():
            for col in B:
                b_msg(col, k, "gm1").wait_recv()
                b_msg(col, k, "ge3").start()
                b_msg(col, k, "gm2").wait_recv()
                b_msg(col, k, "ge4").start()

        @pl.when(is_end)
        def _():
            for col in A:
                a_msg(col, k, "gy").wait_recv()
                a_msg(col, k, "gx2").start()

    def h8(k):
        for col in A:
            a_msg(col, k, "gx1").wait_recv()
            a_msg(col, k, "gx2").wait_recv()

        @pl.when(is_end)
        def _():
            for col in B:
                for what in ("ge1", "ge2", "ge3", "ge4"):
                    b_msg(col, k, what).wait_recv()
        c_msg(k).start()

    def h9(k):
        c_msg(k).wait()
        for col in A:
            for what in ("gy", "gx1", "gx2"):
                a_msg(col, k, what).wait_send()

        @pl.when(is_mid)
        def _():
            for col in A:
                a_msg(col, k, "ge").wait_send()
            for col in B:
                for what in ("gx", "gm1", "gm2", "ge1", "ge2", "ge3", "ge4"):
                    b_msg(col, k, what).wait_send()

    handlers = [h1, h2, h3, h4, h5, h6, h7, h8, h9]
    nh = len(handlers)

    def run(s, t):
        k = t - 1 - s

        @pl.when((k >= 0) & (k < n))
        def _():
            handlers[s - 1](k)

    def tick(t, carry):
        order = list(range(nh, 0, -1))
        for i in range(nb):
            take = order[i * nh // nb:(i + 1) * nh // nb]
            for s in take:
                run(s, t)

            @pl.when(t < n)
            def _(i=i):
                if i == 0:
                    xcopy(t).wait()

                    @pl.when(t + 1 < n)
                    def _():
                        xcopy(t + 1).start()

                @pl.when(t == 0)
                def _():
                    wcopy(i, 0).wait()
                    wcopy(i, 1).wait()
                gu = jnp.dot(xb[lax.rem(t, 2)], wgu[i], preferred_element_type=F32)
                hb[lax.rem(t, 4), :, pl.ds(i * 128, 128)] = (
                    jax.nn.gelu(gu[:, :128]) * gu[:, 128:]).astype(BF16)

        @pl.when(t < n)
        def _():
            h_msg(t).start()

        @pl.when((t >= 1) & (t <= n))
        def _():
            k = t - 1

            @pl.when(t == 1)
            def _():
                wd_own().wait()
                wd_part().wait()
            h_msg(k).wait()
            s = lax.rem(k, W)
            for j in range(half // 256):
                tb[s, :, pl.ds(j * 256, 256)] = jnp.dot(
                    hb[lax.rem(k, 4)], wdv[:, pl.ds(j * 256, 256)], preferred_element_type=F32)
            h0(k)
        return carry

    lax.fori_loop(0, n + 1 + nh, tick, 0)


def solution(mesh):
    def step(x, w_gate, w_up, w_down):
        rows, d = x.shape
        ff = w_gate.shape[1]
        n, half = rows // R, d // 2
        aw, bw = 128 * sum(A_BLOCKS), 128 * sum(B_BLOCKS)
        assert aw + bw == half
        anyspec = pl.BlockSpec(memory_space=pl.ANY)
        ntypes = 44
        W = 5
        return pl.pallas_call(
            functools.partial(kernel, (rows, d, ff)),
            out_shape=jax.ShapeDtypeStruct((rows, d), BF16),
            in_specs=[anyspec] * 4,
            out_specs=anyspec,
            scratch_shapes=[
                pltpu.VMEM((ff // 128, d, 256), BF16),
                pltpu.VMEM((2 * ff, half), BF16),
                pltpu.VMEM((2, R, d), BF16),
                pltpu.VMEM((4, R, 2 * ff), BF16),
                pltpu.VMEM((W, R, half), F32),
                pltpu.VMEM((W, R, half), BF16),
                pltpu.VMEM((W, R // 8, half), BF16),
                pltpu.VMEM((n, R // 2, aw), BF16),
                pltpu.VMEM((n, R // 4, aw), BF16),
                pltpu.VMEM((n, R // 4, aw), BF16),
                pltpu.VMEM((n, R // 8, aw), BF16),
                pltpu.VMEM((n, R, bw), BF16),
                pltpu.VMEM((n, R // 2, bw), BF16),
                pltpu.VMEM((n, R // 4, bw), BF16),
                pltpu.VMEM((n, R // 8, bw), BF16),
                pltpu.SemaphoreType.DMA((2 * (ff // 128) + 1,)),
                pltpu.SemaphoreType.DMA((2,)),
                pltpu.SemaphoreType.DMA((4, n)),
                pltpu.SemaphoreType.DMA((ntypes, n)),
                pltpu.SemaphoreType.DMA((ntypes, n)),
            ],
            compiler_params=pltpu.CompilerParams(
                collective_id=0, has_side_effects=True, vmem_limit_bytes=67043328),
        )(x, w_gate, w_up, w_down)

    return jax.shard_map(
        step,
        mesh=mesh,
        in_specs=(P("dp", None), P(None, "tp"), P(None, "tp"), P("tp", None)),
        out_specs=P("dp", None),
        check_vma=False,
    )
```

```python
import functools

import jax
import jax.numpy as jnp
from jax import lax
from jax.experimental import pallas as pl
from jax.experimental.pallas import tpu as pltpu
from jax.sharding import PartitionSpec as P

MESH = pl.DeviceIdType.MESH
F32, BF16 = jnp.float32, jnp.bfloat16

R = 128

VMEM_LIMIT = 37 * 2**20

A_BLOCKS = (7, 7)
B_BLOCKS = (2, 2)


def kernel(dims, x_ref, wg_ref, wu_ref, wd_ref, y_ref, wgu,
           wdv, xb, hb, tb, stg, fin, rx1, rx2, rz1, rz2, rbz, rbm, rb1, rb2,
           wsem, xsem, ysem, vsem, ss, rs):
    rows, d, ff = dims
    n = rows // R
    half = d // 2
    nb = ff // 128
    W = tb.shape[0]
    me = lax.axis_index("tp")
    c = lax.rem(me, 2)
    z = lax.rem(me // 2, 4)
    yy = lax.rem(me // 8, 2)
    xx = me // 16

    def dev(px, py, pz, pc):
        return ((px * 2 + py) * 4 + pz) * 2 + pc

    xp = dev(1 - xx, yy, z, c)
    yp = dev(xx, 1 - yy, z, c)
    cp = dev(xx, yy, z, 1 - c)
    is_mid = (z == 1) | (z == 2)
    is_end = (z == 0) | (z == 3)
    m = z // 2
    om = dev(xx, yy, 3 - z, c)
    ez = dev(xx, yy, 3 * m, c)
    mz = dev(xx, yy, 1 + m, c)

    ids = {}

    def rc(name, k, src, dst, to):
        i = ids.setdefault(name, len(ids))
        return pltpu.make_async_remote_copy(
            src_ref=src, dst_ref=dst, send_sem=ss.at[i, k], recv_sem=rs.at[i, k],
            device_id={"tp": to}, device_id_type=MESH)

    def wcopy(i, part):
        src = (wg_ref, wu_ref)[part].at[:, pl.ds(i * 128, 128)]
        return pltpu.make_async_copy(src, wgu.at[pl.ds(i * d, d), pl.ds(part * 128, 128)], wsem.at[2 * i + part])

    def xcopy(k):
        return pltpu.make_async_copy(
            x_ref.at[pl.ds(pl.multiple_of(k * R, R), R), :], xb.at[lax.rem(k, 2)], xsem.at[lax.rem(k, 2)])

    def wd_own():
        return pltpu.make_async_copy(
            wd_ref.at[:, pl.ds(pl.multiple_of(c * half, 128), half)], wdv.at[pl.ds(0, ff)], wsem.at[2 * nb])

    def wd_part():
        return rc("wd", 0, wd_ref.at[:, pl.ds(pl.multiple_of((1 - c) * half, 128), half)],
                  wdv.at[pl.ds(ff, ff)], cp)

    xcopy(0).start()
    for i in range(nb):
        for part in range(2):
            wcopy(i, part).start()
    wd_own().start()

    bar = pltpu.get_barrier_semaphore()
    for peer in (xp, yp, cp):
        pl.semaphore_signal(bar, inc=1, device_id={"tp": peer}, device_id_type=MESH)

    @pl.when(is_mid)
    def _():
        pl.semaphore_signal(bar, inc=1, device_id={"tp": om}, device_id_type=MESH)
        pl.semaphore_signal(bar, inc=1, device_id={"tp": ez}, device_id_type=MESH)
        pl.semaphore_wait(bar, 5)

    @pl.when(is_end)
    def _():
        pl.semaphore_signal(bar, inc=1, device_id={"tp": mz}, device_id_type=MESH)
        pl.semaphore_wait(bar, 4)

    wd_part().start()

    A, B = [], []
    off = 0
    for j, blocks in enumerate(A_BLOCKS):
        ax = (xp, xx, yp, yy) if j == 0 else (yp, yy, xp, xx)
        A.append((f"A{j}", off, blocks * 128) + ax)
        off += blocks * 128
    boff = off
    for j, blocks in enumerate(B_BLOCKS):
        ax = (xp, xx, yp, yy) if j == 0 else (yp, yy, xp, xx)
        B.append((f"B{j}", off, blocks * 128) + ax)
        off += blocks * 128
    bw = off - boff
    R2, R4, R8 = R // 2, R // 4, R // 8
    bcols = pl.ds(boff, bw)

    def Y(k, row, nrows, o, w):
        return y_ref.at[pl.ds(pl.multiple_of(k * R + row, 16), nrows),
                        pl.ds(pl.multiple_of(c * half + o, 128), w)]

    def rows_at(start, size):
        return pl.ds(pl.multiple_of(start, 16), size)

    def a_msg(col, k, what):
        nm, o, w, p, a, q, b = col
        s = lax.rem(k, W)
        cols = pl.ds(o, w)
        q0 = a * R2 + b * R4
        key = nm + what
        if what == "xs":
            return rc(key, k, stg.at[s, pl.ds(0, R2), cols], rx1.at[k, :, cols], p)
        if what == "ys":
            return rc(key, k, stg.at[s, pl.ds(R2, R4), cols], rx2.at[k, :, cols], q)
        if what == "ze":
            return rc(key, k, stg.at[s, pl.ds(3 * R4, R4), cols], rz1.at[k, :, cols], mz)
        if what == "zm":
            return rc(key, k, stg.at[s, pl.ds(3 * R4, R8), cols], rz2.at[k, :, cols], om)
        if what == "gm":
            return rc(key, k, fin.at[s, :, cols], Y(k, q0 + m * R8, R8, o, w), om)
        reg = Y(k, q0, R4, o, w)
        if what == "ge":
            return rc(key, k, reg, reg, ez)
        if what == "gy":
            return rc(key, k, reg, reg, q)
        if what == "gx1":
            return rc(key, k, reg, reg, p)
        reg = Y(k, a * R2 + (1 - b) * R4, R4, o, w)
        assert what == "gx2"
        return rc(key, k, reg, reg, p)

    def b_msg(col, k, what):
        nm, o, w, p, a, q, b = col
        s = lax.rem(k, W)
        cols = pl.ds(o, w)
        lc = pl.ds(o - boff, w)
        key = nm + what
        if what == "xs":
            return rc(key, k, stg.at[s, pl.ds(R2, R4), cols], rb1.at[k, :, lc], p)
        if what == "ys":
            return rc(key, k, stg.at[s, pl.ds(3 * R4, R8), cols], rb2.at[k, :, lc], q)
        own = m * R2 + a * R4
        if what == "gy":
            return rc(key, k, fin.at[s, :, cols], Y(k, own + b * R8, R8, o, w), q)
        if what in ("gx", "gm1", "ge1"):
            reg = Y(k, own, R4, o, w)
            return rc(key, k, reg, reg, {"gx": p, "gm1": om, "ge1": ez}[what])
        if what in ("gm2", "ge2"):
            reg = Y(k, m * R2 + (1 - a) * R4, R4, o, w)
            return rc(key, k, reg, reg, {"gm2": om, "ge2": ez}[what])
        row = (1 - m) * R2 + {"ge3": a, "ge4": 1 - a}[what] * R4
        reg = Y(k, row, R4, o, w)
        return rc(key, k, reg, reg, ez)

    def bz_msg(k, what):
        s = lax.rem(k, W)
        if what == "ze":
            return rc("Bze", k, stg.at[s, :, bcols], rbz.at[k], mz)
        return rc("Bzm", k, stg.at[s, pl.ds(0, R2), bcols], rbm.at[k], om)

    def c_msg(k):
        reg = Y(k, 0, R, 0, half)
        return rc("cg", k, reg, reg, cp)

    def h_msg(k):
        sl = lax.rem(k, 4)
        return rc("h", k, hb.at[sl, :, pl.ds(0, ff)], hb.at[sl, :, pl.ds(ff, ff)], cp)

    def to_vmem(k, j):
        r0 = pl.multiple_of(k * R, R)
        return pltpu.make_async_copy(
            y_ref.at[pl.ds(r0, R), pl.ds(j * 256, 256)],
            wgu.at[pl.ds(pl.multiple_of(j * rows + r0, R), R), :], vsem.at[k, j])

    def ylocal(col, j, k, row):
        nm, o, w = col[:3]
        s = lax.rem(k, W)
        return pltpu.make_async_copy(fin.at[s, :, pl.ds(o, w)], Y(k, row, R8, o, w), ysem.at[j, k])

    def a_fin_row(col):
        return col[4] * R2 + col[6] * R4 + m * R8

    def b_fin_row(col):
        return m * R2 + col[4] * R4 + col[6] * R8

    def h0(k):
        s = lax.rem(k, W)
        for col in A:
            nm, o, w, p, a, q, b = col
            cols = pl.ds(o, w)
            stg[s, pl.ds(0, R2), cols] = tb[s, rows_at((1 - a) * R2, R2), cols].astype(BF16)
            a_msg(col, k, "xs").start()

        @pl.when(is_end)
        def _():
            stg[s, :, bcols] = tb[s, :, bcols].astype(BF16)
            bz_msg(k, "ze").start()

    def h1(k):
        s = lax.rem(k, W)
        for col in A:
            nm, o, w, p, a, q, b = col
            cols = pl.ds(o, w)
            a_msg(col, k, "xs").wait_recv()
            snd, kp = (1 - b) * R4, b * R4
            stg[s, pl.ds(R2, R4), cols] = (
                tb[s, rows_at(a * R2 + snd, R4), cols]
                + rx1[k, rows_at(snd, R4), cols].astype(F32)).astype(BF16)
            a_msg(col, k, "ys").start()
            tb[s, rows_at(a * R2 + kp, R4), cols] += rx1[k, rows_at(kp, R4), cols].astype(F32)

        @pl.when(is_mid)
        def _():
            bz_msg(k, "ze").wait_recv()
            stg[s, pl.ds(0, R2), bcols] = (
                tb[s, rows_at((1 - m) * R2, R2), bcols]
                + rbz[k, rows_at((1 - m) * R2, R2), :].astype(F32)).astype(BF16)
            bz_msg(k, "zm").start()
            tb[s, rows_at(m * R2, R2), bcols] += rbz[k, rows_at(m * R2, R2), :].astype(F32)

    def h2(k):
        s = lax.rem(k, W)
        for col in A:
            nm, o, w, p, a, q, b = col
            cols = pl.ds(o, w)
            a_msg(col, k, "ys").wait_recv()
            q0 = rows_at(a * R2 + b * R4, R4)

            @pl.when(is_end)
            def _():
                stg[s, pl.ds(3 * R4, R4), cols] = (
                    tb[s, q0, cols] + rx2[k, :, cols].astype(F32)).astype(BF16)
                a_msg(col, k, "ze").start()

            @pl.when(is_mid)
            def _():
                tb[s, q0, cols] += rx2[k, :, cols].astype(F32)

        @pl.when(is_mid)
        def _():
            bz_msg(k, "zm").wait_recv()
            for col in B:
                nm, o, w, p, a, q, b = col
                cols, lc = pl.ds(o, w), pl.ds(o - boff, w)
                snd, kp = (1 - a) * R4, a * R4
                stg[s, pl.ds(R2, R4), cols] = (
                    tb[s, rows_at(m * R2 + snd, R4), cols]
                    + rbm[k, rows_at(snd, R4), lc].astype(F32)).astype(BF16)
                b_msg(col, k, "xs").start()
                tb[s, rows_at(m * R2 + kp, R4), cols] += rbm[k, rows_at(kp, R4), lc].astype(F32)

    def h3(k):
        s = lax.rem(k, W)

        @pl.when(is_mid)
        def _():
            for col in A:
                nm, o, w, p, a, q, b = col
                cols = pl.ds(o, w)
                a_msg(col, k, "ze").wait_recv()
                q0 = a * R2 + b * R4
                snd, kp = (1 - m) * R8, m * R8
                stg[s, pl.ds(3 * R4, R8), cols] = (
                    tb[s, rows_at(q0 + snd, R8), cols]
                    + rz1[k, rows_at(snd, R8), cols].astype(F32)).astype(BF16)
                a_msg(col, k, "zm").start()
                tb[s, rows_at(q0 + kp, R8), cols] += rz1[k, rows_at(kp, R8), cols].astype(F32)
            for col in B:
                nm, o, w, p, a, q, b = col
                cols, lc = pl.ds(o, w), pl.ds(o - boff, w)
                b_msg(col, k, "xs").wait_recv()
                q0 = m * R2 + a * R4
                snd, kp = (1 - b) * R8, b * R8
                stg[s, pl.ds(3 * R4, R8), cols] = (
                    tb[s, rows_at(q0 + snd, R8), cols]
                    + rb1[k, rows_at(snd, R8), lc].astype(F32)).astype(BF16)
                b_msg(col, k, "ys").start()
                tb[s, rows_at(q0 + kp, R8), cols] += rb1[k, rows_at(kp, R8), lc].astype(F32)

    def h4(k):
        s = lax.rem(k, W)

        @pl.when(is_mid)
        def _():
            for j, col in enumerate(A):
                nm, o, w, p, a, q, b = col
                cols = pl.ds(o, w)
                a_msg(col, k, "zm").wait_recv()
                fin[s, :, cols] = (
                    tb[s, rows_at(a_fin_row(col), R8), cols] + rz2[k, :, cols].astype(F32)).astype(BF16)
                a_msg(col, k, "gm").start()
                ylocal(col, j, k, a_fin_row(col)).start()
            for j, col in enumerate(B):
                nm, o, w, p, a, q, b = col
                cols, lc = pl.ds(o, w), pl.ds(o - boff, w)
                b_msg(col, k, "ys").wait_recv()
                fin[s, :, cols] = (
                    tb[s, rows_at(b_fin_row(col), R8), cols] + rb2[k, :, lc].astype(F32)).astype(BF16)
                b_msg(col, k, "gy").start()
                ylocal(col, 2 + j, k, b_fin_row(col)).start()

    def h5(k):
        @pl.when(is_mid)
        def _():
            for j, col in enumerate(A):
                ylocal(col, j, k, a_fin_row(col)).wait()
                a_msg(col, k, "gm").wait_recv()
                for what in ("ge", "gy", "gx1"):
                    a_msg(col, k, what).start()
            for j, col in enumerate(B):
                ylocal(col, 2 + j, k, b_fin_row(col)).wait()
                b_msg(col, k, "gy").wait_recv()
                for what in ("gx", "gm1", "ge1"):
                    b_msg(col, k, what).start()
            for col in A:
                for what in ("xs", "ys", "zm", "gm"):
                    a_msg(col, k, what).wait_send()
            bz_msg(k, "zm").wait_send()
            for col in B:
                for what in ("xs", "ys", "gy"):
                    b_msg(col, k, what).wait_send()

        @pl.when(is_end)
        def _():
            for col in A:
                for what in ("xs", "ys", "ze"):
                    a_msg(col, k, what).wait_send()
            bz_msg(k, "ze").wait_send()

    def h6(k):
        @pl.when(is_mid)
        def _():
            for col in A:
                a_msg(col, k, "gy").wait_recv()
                a_msg(col, k, "gx2").start()
            for col in B:
                b_msg(col, k, "gx").wait_recv()
                b_msg(col, k, "gm2").start()
                b_msg(col, k, "ge2").start()

        @pl.when(is_end)
        def _():
            for col in A:
                a_msg(col, k, "ge").wait_recv()
                a_msg(col, k, "gy").start()
                a_msg(col, k, "gx1").start()

    def h7(k):
        @pl.when(is_mid)
        def _():
            for col in B:
                b_msg(col, k, "gm1").wait_recv()
                b_msg(col, k, "ge3").start()
                b_msg(col, k, "gm2").wait_recv()
                b_msg(col, k, "ge4").start()

        @pl.when(is_end)
        def _():
            for col in A:
                a_msg(col, k, "gy").wait_recv()
                a_msg(col, k, "gx2").start()

    def h8(k):
        for col in A:
            a_msg(col, k, "gx1").wait_recv()
            a_msg(col, k, "gx2").wait_recv()

        @pl.when(is_end)
        def _():
            for col in B:
                for what in ("ge1", "ge2", "ge3", "ge4"):
                    b_msg(col, k, what).wait_recv()
        c_msg(k).start()

    def h9(k):
        c_msg(k).wait()
        for col in A:
            for what in ("gy", "gx1", "gx2"):
                a_msg(col, k, what).wait_send()

        @pl.when(is_mid)
        def _():
            for col in A:
                a_msg(col, k, "ge").wait_send()
            for col in B:
                for what in ("gx", "gm1", "gm2", "ge1", "ge2", "ge3", "ge4"):
                    b_msg(col, k, what).wait_send()

    handlers = [h1, h2, h3, h4, h5, h6, h7, h8, h9]
    nh = len(handlers)

    def run(t, *stages):
        for s in stages:
            k = t - 1 - s

            @pl.when((k >= 0) & (k < n))
            def _(s=s, k=k):
                handlers[s - 1](k)

    def gateup(t, lo, hi, first):
        for i in range(lo, hi):
            if first:
                wcopy(i, 0).wait()
                wcopy(i, 1).wait()
            gu = jnp.dot(xb[lax.rem(t, 2)], wgu[pl.ds(i * d, d), :], preferred_element_type=F32)
            hb[lax.rem(t, 4), :, pl.ds(i * 128, 128)] = (
                jax.nn.gelu(gu[:, :128]) * gu[:, 128:]).astype(BF16)

    def down(k):
        h_msg(k).wait()
        s = lax.rem(k, W)
        for j in range(half // 256):
            tb[s, :, pl.ds(j * 256, 256)] = jnp.dot(
                hb[lax.rem(k, 4)], wdv[:, pl.ds(j * 256, 256)], preferred_element_type=F32)

    xcopy(0).wait()
    xcopy(1).start()
    gateup(0, 0, nb, True)
    h_msg(0).start()
    wd_own().wait()
    wd_part().wait()

    def tick(t, carry):
        run(t, 9, 8, 7, 6)
        xcopy(t).wait()

        @pl.when(t + 1 < n)
        def _():
            xcopy(t + 1).start()
        gateup(t, 0, 5, False)
        run(t, 5, 4, 3)
        gateup(t, 5, nb, False)
        h_msg(t).start()
        down(t - 1)
        run(t, 2, 1)
        h0(t - 1)
        return carry

    lax.fori_loop(1, n, tick, 0)
    down(n - 1)
    run(n, 9, 8, 7, 6, 5, 4, 3, 2, 1)
    h0(n - 1)

    def fetch(k):
        for j in range(d // 256):
            to_vmem(k, j).start()

    early = n - nh

    def fetch_early(k, carry):
        fetch(k)
        return carry

    lax.fori_loop(0, early, fetch_early, 0)

    def drain(t, carry):
        run(t, 9, 8, 7, 6, 5, 4, 3, 2, 1)
        fetch(t - 1 - nh)
        return carry

    lax.fori_loop(n + 1, n + 1 + nh, drain, 0)

    def fetched(k, carry):
        for j in range(d // 256):
            to_vmem(k, j).wait()
        return carry

    lax.fori_loop(0, n, fetched, 0)


def store_kernel(v_ref, o_ref, sem):
    rows, d = o_ref.shape
    copies = [
        pltpu.make_async_copy(
            v_ref.at[pl.ds(j * rows, rows), :], o_ref.at[:, pl.ds(j * 256, 256)], sem.at[j])
        for j in range(d // 256)]
    for c in copies:
        c.start()
    for c in copies:
        c.wait()


def solution(mesh):
    def step(x, w_gate, w_up, w_down):
        rows, d = x.shape
        ff = w_gate.shape[1]
        n, half = rows // R, d // 2
        aw, bw = 128 * sum(A_BLOCKS), 128 * sum(B_BLOCKS)
        assert aw + bw == half
        anyspec = pl.BlockSpec(memory_space=pl.ANY)
        ntypes = 44
        W = 5
        _, v = pl.pallas_call(
            functools.partial(kernel, (rows, d, ff)),
            out_shape=[jax.ShapeDtypeStruct((rows, d), BF16),
                       pltpu.VMEM((ff // 128 * d, 256), BF16)],
            in_specs=[anyspec] * 4,
            out_specs=[anyspec, pl.BlockSpec(memory_space=pltpu.VMEM)],
            scratch_shapes=[
                pltpu.VMEM((2 * ff, half), BF16),
                pltpu.VMEM((2, R, d), BF16),
                pltpu.VMEM((4, R, 2 * ff), BF16),
                pltpu.VMEM((W, R, half), F32),
                pltpu.VMEM((W, R, half), BF16),
                pltpu.VMEM((W, R // 8, half), BF16),
                pltpu.VMEM((n, R // 2, aw), BF16),
                pltpu.VMEM((n, R // 4, aw), BF16),
                pltpu.VMEM((n, R // 4, aw), BF16),
                pltpu.VMEM((n, R // 8, aw), BF16),
                pltpu.VMEM((n, R, bw), BF16),
                pltpu.VMEM((n, R // 2, bw), BF16),
                pltpu.VMEM((n, R // 4, bw), BF16),
                pltpu.VMEM((n, R // 8, bw), BF16),
                pltpu.SemaphoreType.DMA((2 * (ff // 128) + 1,)),
                pltpu.SemaphoreType.DMA((2,)),
                pltpu.SemaphoreType.DMA((4, n)),
                pltpu.SemaphoreType.DMA((n, d // 256)),
                pltpu.SemaphoreType.DMA((ntypes, n)),
                pltpu.SemaphoreType.DMA((ntypes, n)),
            ],
            compiler_params=pltpu.CompilerParams(
                collective_id=0, has_side_effects=True, vmem_limit_bytes=VMEM_LIMIT),
        )(x, w_gate, w_up, w_down)
        return pl.pallas_call(
            store_kernel,
            out_shape=jax.ShapeDtypeStruct((rows, d), BF16),
            in_specs=[pl.BlockSpec(memory_space=pltpu.VMEM)],
            out_specs=anyspec,
            scratch_shapes=[pltpu.SemaphoreType.DMA((d // 256,))],
            compiler_params=pltpu.CompilerParams(vmem_limit_bytes=2**20),
        )(v)

    return jax.shard_map(
        step,
        mesh=mesh,
        in_specs=(P("dp", None), P(None, "tp"), P(None, "tp"), P("tp", None)),
        out_specs=P("dp", None),
        check_vma=False,
    )
```
